768 devices in a mesh: section: 16 (over x, y_hi, core), mp: 48 (over z, y_lo).
Axes of the slice: x: 4, y: 8 (y_hi: 2, y_lo: 4; y = y_hi * 4 + y_lo), z: 12, core: 2. Of those that a mesh axis runs over, the one named last changes fastest.
Arguments:
- encoder_input: bfloat16 [2304, 1024], P('section'), may hold values from -6 to 6
- input_gain: float32 [1024], replicated, may hold values from 0.1 to 1.9
- expand_weight: bfloat16 [1024, 49152], P(None, 'mp'), may hold values from -0.1875 to 0.1875
- reduce_weight: bfloat16 [49152, 1024], P('mp'), may hold values from -0.02734375 to 0.02734375
- final_gain: float32 [1024], replicated, may hold values from 0.1 to 1.9
- decoder_input: bfloat16 [4096, 1024], P('section'), may hold values from -6 to 6
- query_gain: float32 [1024], replicated, may hold values from 0.1 to 1.9
- query_weight: bfloat16 [1024, 12288], P(None, 'mp'), may hold values from -2 to 2
- key_weight: bfloat16 [1024, 12288], P(None, 'mp'), may hold values from -0.1875 to 0.1875
- value_weight: bfloat16 [1024, 12288], P(None, 'mp'), may hold values from -0.1875 to 0.1875
- mixing_weight: bfloat16 [12288, 1024], P('mp'), may hold values from -0.0546875 to 0.0546875
- output_gradient: bfloat16 [4096, 1024], P('section'), may hold values from -342 to 342
Outputs:
- memory: bfloat16 [2304, 1024], P(('section', 'mp'))
- memory_gradient: bfloat16 [2304, 1024], P(('section', 'mp'))
The draws below stay inside these ranges and needn't reach their ends.
All inputs are finite; a program needn't handle non-finite values.
Results may differ from the reference program's by a relative error of at most 0.025.
The reference program's roundings to bfloat16 on the way (of `normed`, `hidden`, `dec_normed`, `queries` and `head_grad`) count: a program that leaves them out, or rounds other values in their place, can miss the bound.
Values may be sent and summed in bfloat16 or wider, within the bound.
A program may use at most 64 MiB of HBM per device.

```python
import jax
import jax.numpy as jnp
from jax import lax

D = 1024
DK = 128
FF = 49152
HEADS = 96
INNER = 12288
ENC_TOTAL = 2304
DEC_TOTAL = 4096


def draw_query_weight(key, part):
    second = jax.random.fold_in(jax.random.fold_in(key, 11), 1)
    values = jax.random.normal(second, (D, INNER), jnp.float32) / D ** 0.5
    values = jnp.clip(values, -6.0 / D ** 0.5, 6.0 / D ** 0.5)
    return jnp.clip(values, -2.0, 2.0).astype(jnp.bfloat16)


def levels(key, dims, cuts, low, high):
    def one(position, shards_of):
        draws = jax.random.uniform(jax.random.fold_in(jax.random.fold_in(key, 6), position), (shards_of,), jnp.float32, low / len(cuts), high / len(cuts))
        return jnp.repeat(jnp.exp(draws), dims[position] // shards_of).reshape((-1,) + (1,) * (len(dims) - position - 1))

    level = one(*cuts[0])
    for cut in cuts[1:]:
        level = level * one(*cut)
    return level


def scatter_about(own_key, dims, scale, reach, cuts=(), kind=jnp.bfloat16):
    values = scale * jax.random.normal(own_key, dims, jnp.float32)
    if cuts:
        values = values * levels(own_key, dims, cuts, -0.22, 0.18)
    return jnp.clip(values, -reach, reach).astype(kind)


def setup_inputs(seed: int = 0) -> dict:
    splits = jax.random.split(jax.random.key(seed), 13)
    encoder_input = scatter_about(splits[0], (ENC_TOTAL, D), 1.0, 6.0, ((0, 16),))
    input_gain = jnp.clip(1.0 + 0.18 * jax.random.normal(splits[1], (D,), jnp.float32), 0.1, 1.9)
    expand_weight = scatter_about(splits[2], (D, FF), D ** -0.5, 0.1875, ((1, 48),))
    reduce_weight = scatter_about(splits[3], (FF, D), FF ** -0.5, 0.02734375, ((0, 48),))
    final_gain = jnp.clip(1.0 + 0.18 * jax.random.normal(splits[4], (D,), jnp.float32), 0.1, 1.9)
    decoder_input = scatter_about(splits[5], (DEC_TOTAL, D), 1.0, 6.0, ((0, 16),))
    query_gain = jnp.clip(1.0 + 0.18 * jax.random.normal(splits[6], (D,), jnp.float32), 0.1, 1.9)
    query_weight = draw_query_weight(jax.random.fold_in(splits[12], 71), 0)
    key_weight = scatter_about(splits[8], (D, INNER), D ** -0.5, 0.1875, ((1, 48),))
    value_weight = scatter_about(splits[9], (D, INNER), D ** -0.5, 0.1875, ((1, 48),))
    mixing_weight = scatter_about(splits[10], (INNER, D), INNER ** -0.5, 0.0546875, ((0, 48),))
    output_gradient = scatter_about(splits[11], (DEC_TOTAL, D), (ENC_TOTAL // 40), 342.0, ((0, 16),))
    return dict(encoder_input=encoder_input, input_gain=input_gain, expand_weight=expand_weight, reduce_weight=reduce_weight, final_gain=final_gain, decoder_input=decoder_input, query_gain=query_gain, query_weight=query_weight, key_weight=key_weight, value_weight=value_weight, mixing_weight=mixing_weight, output_gradient=output_gradient)


def norm_rows(rows, gain):
    values = rows.astype(jnp.float32)
    return values * lax.rsqrt(lax.optimization_barrier(jnp.mean(values * values, axis=-1, keepdims=True)) + 1e-06) * gain

def one_head(operands):
    query_block, key_block, value_block, grad_block = operands
    scale = DK ** (-0.5)
    scores = jnp.dot(query_block, key_block.T, preferred_element_type=jnp.float32) * scale
    probs = jax.nn.softmax(scores, axis=-1)
    prob_grad = jnp.dot(grad_block, value_block.T, preferred_element_type=jnp.float32)
    delta = lax.optimization_barrier(jnp.sum(probs * prob_grad, axis=-1, keepdims=True))
    score_grad = (probs * (prob_grad - delta) * scale).astype(jnp.bfloat16)
    probs_low = probs.astype(jnp.bfloat16)
    key_grad = jnp.dot(score_grad.T, query_block, preferred_element_type=jnp.float32).astype(jnp.bfloat16)
    value_grad = jnp.dot(probs_low.T, grad_block, preferred_element_type=jnp.float32).astype(jnp.bfloat16)
    return (key_grad, value_grad)

def split_heads(matrix):
    return matrix.reshape(matrix.shape[0], HEADS, DK).transpose(1, 0, 2)

def reference(encoder_input, input_gain, expand_weight, reduce_weight, final_gain, decoder_input, query_gain, query_weight, key_weight, value_weight, mixing_weight, output_gradient):
    normed = norm_rows(encoder_input, input_gain).astype(jnp.bfloat16)
    hidden = jnp.maximum(jnp.dot(normed, expand_weight, preferred_element_type=jnp.float32), 0.0).astype(jnp.bfloat16)
    residual_sum = encoder_input.astype(jnp.float32) + jnp.dot(hidden, reduce_weight, preferred_element_type=jnp.float32)
    memory = norm_rows(residual_sum, final_gain).astype(jnp.bfloat16)
    dec_normed = norm_rows(decoder_input, query_gain).astype(jnp.bfloat16)
    queries = jnp.dot(dec_normed, query_weight, preferred_element_type=jnp.float32).astype(jnp.bfloat16)
    keys = jnp.dot(memory, key_weight, preferred_element_type=jnp.float32).astype(jnp.bfloat16)
    values = jnp.dot(memory, value_weight, preferred_element_type=jnp.float32).astype(jnp.bfloat16)
    head_grad = jnp.dot(output_gradient, mixing_weight.T, preferred_element_type=jnp.float32).astype(jnp.bfloat16)
    key_heads, value_heads = lax.map(one_head, (split_heads(queries), split_heads(keys), split_heads(values), split_heads(head_grad)))
    key_grad = key_heads.transpose(1, 0, 2).reshape(keys.shape[0], HEADS * DK)
    value_grad = value_heads.transpose(1, 0, 2).reshape(keys.shape[0], HEADS * DK)
    memory_gradient = jnp.dot(key_grad, key_weight.T, preferred_element_type=jnp.float32) + jnp.dot(value_grad, value_weight.T, preferred_element_type=jnp.float32)
    return (memory, memory_gradient.astype(jnp.bfloat16))
```

```python
import jax
import jax.numpy as jnp
from jax import lax
from jax.experimental import pallas as pl
from jax.experimental.pallas import tpu as pltpu
from jax.sharding import PartitionSpec as P

DK = 128
D = 1024
CHUNKS = D // 128
MP = 48
ROWS = 144
SHARE = ROWS // MP
PIECE = SHARE * CHUNKS
QROWS = 256
QALL = 4096
BLOCK = 512
BLOCKS = QALL // BLOCK
WIDTH = 2 * DK
SCALE = DK ** (-0.5)
BF = jnp.bfloat16
F32 = jnp.float32


def dot(a, b):
    return jnp.dot(a, b, preferred_element_type=F32)


def dot_t(a, b):
    return lax.dot_general(a, b, (((1,), (1,)), ((), ())), preferred_element_type=F32)


def norm_rows(rows, gain):
    values = rows.astype(F32)
    return values * lax.rsqrt(jnp.mean(values * values, axis=-1, keepdims=True) + 1e-06) * gain


def merge(a, b):
    top = jnp.maximum(a[0], b[0])
    left = jnp.exp(a[0] - top)
    right = jnp.exp(b[0] - top)
    return top, a[1] * left + b[1] * right, a[2] * left + b[2] * right


def kernel(
    x_hbm, ig_ref, we_hbm, wr_hbm, fg_ref, dec_hbm, qg_ref, wq_hbm, wk_hbm, wv_hbm, mix_hbm, og_hbm,
    mem_out, grad_out,
    x_v, we_v, wr_v, dec_v, wq_v, wk_v, wv_v, mix_v, og_v, load_sem,
    wide, stage, own, res, send, recv, send2, recv2, gath, mem,
    qg, wts, pgr, stats, got_d, mid, got_y, pair, got_x, fin,
    rs_s, rs_r, ag_s, ag_r, rs2_s, rs2_r,
    y_s, y_r, x_s, x_r, h_s, h_r, d_s, d_r,
    sd_s, sd_r, sy_s, sy_r, sx_s, sx_r, sf_s, sf_r,
):
    sec = lax.axis_index("section")
    me = lax.axis_index("mp")
    xi = sec // 4
    yi = (sec // 2) % 2
    core = sec % 2

    def section_of(dx, dy, dc):
        return (((xi + dx) % 4) * 2 + (yi + dy) % 2) * 2 + (core + dc) % 2

    ypeer, dpeer = section_of(0, 1, 0), section_of(0, 0, 1)
    right, left, across = section_of(1, 0, 0), section_of(3, 0, 0), section_of(2, 0, 0)

    def remote(src, dst, ss, rs, s, m):
        return pltpu.make_async_remote_copy(
            src_ref=src, dst_ref=dst, send_sem=ss, recv_sem=rs, device_id=(s, m),
            device_id_type=pl.DeviceIdType.MESH,
        )

    barrier = pltpu.get_barrier_semaphore()

    def greet(k, carry):
        pl.semaphore_signal(
            barrier, inc=1, device_id=(sec, (me + k) % MP), device_id_type=pl.DeviceIdType.MESH
        )
        return carry

    lax.fori_loop(1, MP, greet, 0)
    for s in (ypeer, dpeer, right, left, across):
        pl.semaphore_signal(
            barrier, inc=1, device_id=(s, me), device_id_type=pl.DeviceIdType.MESH
        )

    loads = [
        pltpu.make_async_copy(a, b, load_sem.at[i])
        for i, (a, b) in enumerate(
            (
                (x_hbm, x_v), (we_hbm, we_v), (wr_hbm, wr_v), (dec_hbm, dec_v), (wq_hbm, wq_v),
                (og_hbm, og_v), (mix_hbm, mix_v), (wk_hbm, wk_v), (wv_hbm, wv_v),
            )
        )
    ]
    for load in loads:
        load.start()

    loads[0].wait()
    normed = norm_rows(x_v[...], ig_ref[...]).astype(BF)
    values = x_v[...].astype(F32)
    for c in range(CHUNKS):
        wide[c] = values[:, c * 128 : (c + 1) * 128]
    for c in range(CHUNKS):
        for r in range(SHARE):
            res[pl.ds(r * CHUNKS + c, 1), :] = wide[c, pl.ds(SHARE * me + r, 1), :]
    loads[1].wait()
    hidden = jnp.maximum(dot(normed, we_v[...]), 0.0).astype(BF)
    loads[2].wait()
    part = dot(hidden, wr_v[...])
    for c in range(CHUNKS):
        wide[c] = part[:, c * 128 : (c + 1) * 128]
    for c in range(CHUNKS):
        for r in range(SHARE):
            stage[pl.ds(r * CHUNKS + c, MP, stride=PIECE), :] = wide[c, pl.ds(r, MP, stride=SHARE), :]
    send[...] = stage[...].reshape(MP, PIECE, 128).astype(BF)

    pl.semaphore_wait(barrier, MP - 1 + 5)

    def scatter(src, dst, ss, rs):
        def one(m):
            remote(src.at[m], dst.at[me], ss, rs, sec, m).start()

        one((me + MP // 2) % MP)

        def both(k, carry):
            d = MP // 2 - 1 - k
            one((me + d) % MP)
            one((me + MP - d) % MP)
            return carry

        lax.fori_loop(0, MP // 2 - 1, both, 0)
        dst[me] = src[me]

    def drained(src, dst, ss, rs):
        return remote(src.at[pl.ds(0, MP - 1)], dst.at[pl.ds(0, MP - 1)], ss, rs, sec, (me + 1) % MP)

    def summed(pieces):
        return jnp.sum(pieces[...].astype(F32), axis=0)

    scatter(send, recv, rs_s, rs_r)

    loads[3].wait()
    dec = norm_rows(dec_v[...], qg_ref[...]).astype(BF)
    loads[4].wait()
    tokens = pl.ds(pl.multiple_of(sec * QROWS, QROWS), QROWS)
    qg[tokens, 0:WIDTH] = dot(dec, wq_v[...]).astype(BF)
    loads[5].wait()
    loads[6].wait()
    qg[tokens, WIDTH : 2 * WIDTH] = dot_t(og_v[...], mix_v[...]).astype(BF)

    def rows_of(s, half=None):
        if half is None:
            return qg.at[pl.ds(pl.multiple_of(s * QROWS, QROWS), QROWS), :]
        return qg.at[pl.ds(pl.multiple_of(s * QROWS + half * (QROWS // 2), QROWS // 2), QROWS // 2), :]

    copies = []

    def forward(s, half, ss, rs, to):
        ref = rows_of(s, half)
        copy = remote(ref, ref, ss, rs, to, me)
        copy.start()
        copies.append(copy)

    def arrival(s, half, ss, rs):
        ref = rows_of(s, half)
        remote(ref, ref, ss, rs, dpeer, me).wait_recv()

    s_me, s_y = sec, ypeer
    s_r, s_l, s_a = right, left, across
    s_ry, s_ly, s_ay = section_of(1, 1, 0), section_of(3, 1, 0), section_of(2, 1, 0)
    forward(s_me, None, y_s, y_r, ypeer)
    forward(s_me, None, x_s.at[0], x_r.at[0], right)
    forward(s_me, None, x_s.at[1], x_r.at[1], left)
    forward(s_me, None, d_s.at[0], d_r.at[0], dpeer)
    arrival(s_l, None, x_s.at[0], x_r.at[0])
    forward(s_l, 0, h_s.at[0], h_r.at[0], right)
    forward(s_l, None, d_s.at[1], d_r.at[1], dpeer)
    arrival(s_r, None, x_s.at[1], x_r.at[1])
    forward(s_r, 1, h_s.at[1], h_r.at[1], left)
    forward(s_r, None, d_s.at[2], d_r.at[2], dpeer)

    rs_copy = drained(send, recv, rs_s, rs_r)
    rs_copy.wait_recv()
    rows = (summed(recv) + res[...]).reshape(SHARE, CHUNKS, 128)
    mean = jnp.sum(jnp.sum(rows * rows, axis=2, keepdims=True), axis=1, keepdims=True) * (1.0 / D)
    rows = rows * lax.rsqrt(mean + 1e-06) * fg_ref[...].reshape(1, CHUNKS, 128)
    own[...] = rows.reshape(PIECE, 128)
    gath[me] = own[...].astype(BF)

    def spread(m):
        remote(gath.at[me], gath.at[me], ag_s, ag_r, sec, m).start()

    spread((me + MP // 2) % MP)

    def both(k, carry):
        d = MP // 2 - 1 - k
        spread((me + d) % MP)
        spread((me + MP - d) % MP)
        return carry

    lax.fori_loop(0, MP // 2 - 1, both, 0)
    for r in range(SHARE):
        for c in range(CHUNKS):
            mem_out[r : r + 1, c * 128 : (c + 1) * 128] = own[
                r * CHUNKS + c : r * CHUNKS + c + 1, :
            ].astype(BF)

    arrival(s_y, None, y_s, y_r)
    forward(s_y, None, x_s.at[2], x_r.at[2], right)
    forward(s_y, None, x_s.at[3], x_r.at[3], left)
    forward(s_y, None, d_s.at[3], d_r.at[3], dpeer)
    arrival(s_a, 0, h_s.at[0], h_r.at[0])
    arrival(s_a, 1, h_s.at[1], h_r.at[1])
    forward(s_a, None, d_s.at[4], d_r.at[4], dpeer)
    arrival(s_ly, None, x_s.at[2], x_r.at[2])
    forward(s_ly, 0, h_s.at[2], h_r.at[2], right)
    forward(s_ly, None, d_s.at[5], d_r.at[5], dpeer)
    arrival(s_ry, None, x_s.at[3], x_r.at[3])
    forward(s_ry, 1, h_s.at[3], h_r.at[3], left)
    forward(s_ry, None, d_s.at[6], d_r.at[6], dpeer)

    ag_copy = drained(gath, gath, ag_s, ag_r)
    ag_copy.wait_recv()
    stage[...] = gath[...].reshape(MP * PIECE, 128).astype(F32)
    for r in range(SHARE):
        for c in range(CHUNKS):
            mem[r * MP : (r + 1) * MP, c * 128 : (c + 1) * 128] = stage[
                pl.ds(r * CHUNKS + c, MP, stride=PIECE), :
            ].astype(BF)
    loads[7].wait()
    keys = dot(mem[...], wk_v[...]).astype(BF)
    loads[8].wait()
    vals = dot(mem[...], wv_v[...]).astype(BF)

    arrival(s_ay, 0, h_s.at[2], h_r.at[2])
    arrival(s_ay, 1, h_s.at[3], h_r.at[3])
    forward(s_ay, None, d_s.at[7], d_r.at[7], dpeer)
    order = (
        section_of(0, 0, 1), section_of(3, 0, 1), section_of(1, 0, 1), section_of(0, 1, 1),
        section_of(2, 0, 1), section_of(3, 1, 1), section_of(1, 1, 1), section_of(2, 1, 1),
    )
    for i, s in enumerate(order):
        arrival(s, None, d_s.at[i], d_r.at[i])

    for h in range(2):
        key_h = keys[:, h * DK : (h + 1) * DK]
        val_h = vals[:, h * DK : (h + 1) * DK]

        def block(b, carry, h=h, key_h=key_h, val_h=val_h):
            at = pl.ds(pl.multiple_of(b * BLOCK, BLOCK), BLOCK)
            s = dot_t(key_h, qg[at, h * DK : (h + 1) * DK]) * SCALE
            pg = dot_t(val_h, qg[at, WIDTH + h * DK : WIDTH + (h + 1) * DK])
            top = jnp.max(s, axis=0, keepdims=True)
            w = jnp.exp(s - top)
            wts[h, b] = w
            pgr[h, b] = pg
            row = pl.ds(b, 1)
            stats[h, 0, row, :] = top
            stats[h, 1, row, :] = jnp.sum(w, axis=0, keepdims=True)
            stats[h, 2, row, :] = jnp.sum(w * pg, axis=0, keepdims=True)
            return carry

        lax.fori_loop(0, BLOCKS, block, 0)

    def three(ref):
        return ref[0], ref[1], ref[2]

    def put(ref, values):
        for i in range(3):
            ref[i] = values[i]

    sd = remote(stats.at[1 - core], got_d, sd_s, sd_r, dpeer, me)
    sd.start()
    sd.wait_recv()
    put(mid, merge(three(stats.at[core]), three(got_d)))
    sy = remote(mid, got_y, sy_s, sy_r, ypeer, me)
    sy.start()
    sy.wait_recv()
    put(pair, merge(three(mid), three(got_y)))
    sx = [
        remote(pair, got_x.at[i], sx_s.at[i], sx_r.at[i], to, me)
        for i, to in enumerate((across, right, left))
    ]
    for copy in sx:
        copy.start()
    sx[1].wait_recv()
    total = merge(three(pair), three(got_x.at[1]))
    sx[2].wait_recv()
    total = merge(total, three(got_x.at[2]))
    sx[0].wait_recv()
    put(fin.at[core], merge(total, three(got_x.at[0])))
    sf = remote(fin.at[core], fin.at[core], sf_s, sf_r, dpeer, me)
    sf.start()
    sf.wait_recv()

    sums = []
    for h in range(2):

        def block(b, carry, h=h):
            at = pl.ds(pl.multiple_of(b * BLOCK, BLOCK), BLOCK)
            row = pl.ds(b, 1)
            total = fin[h, 1, row, :]
            factor = jnp.exp(stats[h, 0, row, :] - fin[h, 0, row, :]) / total
            delta = fin[h, 2, row, :] / total
            probs = wts[h, b] * factor
            sg = (probs * (pgr[h, b] - delta) * SCALE).astype(BF)
            kg = carry[0] + dot(sg, qg[at, h * DK : (h + 1) * DK])
            vg = carry[1] + dot(probs.astype(BF), qg[at, WIDTH + h * DK : WIDTH + (h + 1) * DK])
            return kg, vg

        zero = jnp.zeros((ROWS, DK), F32)
        sums.append(lax.fori_loop(0, BLOCKS, block, (zero, zero)))
    kg = jnp.concatenate([s[0] for s in sums], axis=1).astype(BF)
    vg = jnp.concatenate([s[1] for s in sums], axis=1).astype(BF)
    part = dot_t(kg, wk_v[...]) + dot_t(vg, wv_v[...])
    for r in range(SHARE):
        for c in range(CHUNKS):
            stage[pl.ds(r * CHUNKS + c, MP, stride=PIECE), :] = part[
                r * MP : (r + 1) * MP, c * 128 : (c + 1) * 128
            ]
    send2[...] = stage[...].reshape(MP, PIECE, 128).astype(BF)
    scatter(send2, recv2, rs2_s, rs2_r)
    rs2_copy = drained(send2, recv2, rs2_s, rs2_r)

    rs_copy.wait_send()
    ag_copy.wait_send()
    for copy in copies + [sd, sy, sf] + sx:
        copy.wait_send()
    rs2_copy.wait_recv()
    own[...] = summed(recv2)
    for r in range(SHARE):
        for c in range(CHUNKS):
            grad_out[r : r + 1, c * 128 : (c + 1) * 128] = own[
                r * CHUNKS + c : r * CHUNKS + c + 1, :
            ].astype(BF)
    rs2_copy.wait_send()


def body(
    encoder_input, input_gain, expand_weight, reduce_weight, final_gain, decoder_input, query_gain,
    query_weight, key_weight, value_weight, mixing_weight, output_gradient,
):
    vmem = pl.BlockSpec(memory_space=pltpu.VMEM)
    hbm = pl.BlockSpec(memory_space=pl.ANY)
    dma = pltpu.SemaphoreType.DMA
    piece3 = (3, BLOCKS, BLOCK)
    out = jax.ShapeDtypeStruct((SHARE, D), BF)
    return pl.pallas_call(
        kernel,
        out_shape=(out, out),
        in_specs=[hbm, vmem, hbm, hbm, vmem, hbm, vmem, hbm, hbm, hbm, hbm, hbm],
        out_specs=(vmem, vmem),
        scratch_shapes=[
            pltpu.VMEM(encoder_input.shape, BF),
            pltpu.VMEM(expand_weight.shape, BF),
            pltpu.VMEM(reduce_weight.shape, BF),
            pltpu.VMEM(decoder_input.shape, BF),
            pltpu.VMEM(query_weight.shape, BF),
            pltpu.VMEM(key_weight.shape, BF),
            pltpu.VMEM(value_weight.shape, BF),
            pltpu.VMEM(mixing_weight.shape, BF),
            pltpu.VMEM(output_gradient.shape, BF),
            dma((9,)),
            pltpu.VMEM((CHUNKS, ROWS, 128), F32),
            pltpu.VMEM((MP * PIECE, 128), F32),
            pltpu.VMEM((PIECE, 128), F32),
            pltpu.VMEM((PIECE, 128), F32),
            pltpu.VMEM((MP, PIECE, 128), BF),
            pltpu.VMEM((MP, PIECE, 128), BF),
            pltpu.VMEM((MP, PIECE, 128), BF),
            pltpu.VMEM((MP, PIECE, 128), BF),
            pltpu.VMEM((MP, PIECE, 128), BF),
            pltpu.VMEM((ROWS, D), BF),
            pltpu.VMEM((QALL, 2 * WIDTH), BF),
            pltpu.VMEM((2, BLOCKS, ROWS, BLOCK), F32),
            pltpu.VMEM((2, BLOCKS, ROWS, BLOCK), F32),
            pltpu.VMEM((2, *piece3), F32),
            pltpu.VMEM(piece3, F32),
            pltpu.VMEM(piece3, F32),
            pltpu.VMEM(piece3, F32),
            pltpu.VMEM(piece3, F32),
            pltpu.VMEM((3, *piece3), F32),
            pltpu.VMEM((2, *piece3), F32),
            dma, dma, dma, dma, dma, dma,
            dma, dma, dma((4,)), dma((4,)), dma((4,)), dma((4,)), dma((8,)), dma((8,)),
            dma, dma, dma, dma, dma((3,)), dma((3,)), dma, dma,
        ],
        compiler_params=pltpu.CompilerParams(
            collective_id=0, has_side_effects=True, vmem_limit_bytes=60 * 1024 * 1024
        ),
    )(
        encoder_input, input_gain.reshape(1, D), expand_weight, reduce_weight,
        final_gain.reshape(CHUNKS, 128), decoder_input, query_gain.reshape(1, D), query_weight,
        key_weight, value_weight, mixing_weight, output_gradient,
    )


def solution(mesh):
    in_specs = (
        P("section", None), P(), P(None, "mp"), P("mp", None), P(), P("section", None), P(),
        P(None, "mp"), P(None, "mp"), P(None, "mp"), P("mp", None), P("section", None),
    )
    out_specs = (P(("section", "mp"), None), P(("section", "mp"), None))
    return jax.shard_map(body, mesh=mesh, in_specs=in_specs, out_specs=out_specs, check_vma=False)
```

```python
import jax
import jax.numpy as jnp
from jax import lax
from jax.experimental import pallas as pl
from jax.experimental.pallas import tpu as pltpu
from jax.sharding import PartitionSpec as P

DK = 128
D = 1024
CHUNKS = D // 128
ZS, YS = 12, 4
MP = ZS * YS
ROWS = 144
SHARE = ROWS // MP
PIECE = SHARE * CHUNKS
HEAD, TAIL = CHUNKS, PIECE - CHUNKS
QROWS = 256
QALL = 4096
BLOCK = 512
BLOCKS = QALL // BLOCK
WIDTH = 2 * DK
SCALE = DK ** (-0.5)
BF = jnp.bfloat16
F32 = jnp.float32


def dot(a, b):
    return jnp.dot(a, b, preferred_element_type=F32)


def dot_t(a, b):
    return lax.dot_general(a, b, (((1,), (1,)), ((), ())), preferred_element_type=F32)


def norm_rows(rows, gain):
    values = rows.astype(F32)
    return values * lax.rsqrt(jnp.mean(values * values, axis=-1, keepdims=True) + 1e-06) * gain


def merge(a, b):
    top = jnp.maximum(a[0], b[0])
    left = jnp.exp(a[0] - top)
    right = jnp.exp(b[0] - top)
    return top, a[1] * left + b[1] * right, a[2] * left + b[2] * right


def kernel(
    x_hbm, ig_ref, we_hbm, wr_hbm, fg_ref, dec_hbm, qg_ref, wq_hbm, wk_hbm, wv_hbm, mix_hbm, og_hbm,
    mem_out, grad_out,
    x_v, we_v, wr_v, dec_v, wq_v, wk_v, wv_v, mix_v, og_v, load_sem,
    wide, stage, own, res, bufs1, bufs2, gath_a, gath_b, mem,
    qg, wts, pgr, stats, got_d, mid, got_y, pair, got_x, fin, grads,
    rs_sems, ag_sems, rs2_sems,
    y_s, y_r, x_s, x_r, d_s, d_r,
    sd_s, sd_r, sy_s, sy_r, sx_s, sx_r, sf_s, sf_r,
):
    sec = lax.axis_index("section")
    me = lax.axis_index("mp")
    xi = sec // 4
    yi = (sec // 2) % 2
    core = sec % 2
    zi, yl = me // YS, me % YS

    def section_of(dx, dy, dc):
        return (((xi + dx) % 4) * 2 + (yi + dy) % 2) * 2 + (core + dc) % 2

    ypeer, dpeer = section_of(0, 1, 0), section_of(0, 0, 1)
    right, left, across = section_of(1, 0, 0), section_of(3, 0, 0), section_of(2, 0, 0)

    def remote(src, dst, ss, rs, s, m):
        return pltpu.make_async_remote_copy(
            src_ref=src, dst_ref=dst, send_sem=ss, recv_sem=rs, device_id=(s, m),
            device_id_type=pl.DeviceIdType.MESH,
        )

    loads = [
        pltpu.make_async_copy(a, b, load_sem.at[i])
        for i, (a, b) in enumerate(
            (
                (x_hbm, x_v), (we_hbm, we_v), (wr_hbm, wr_v), (dec_hbm, dec_v), (wq_hbm, wq_v),
                (og_hbm, og_v), (mix_hbm, mix_v), (wk_hbm, wk_v), (wv_hbm, wv_v),
            )
        )
    ]
    for load in loads:
        load.start()

    barrier = pltpu.get_barrier_semaphore()

    def greet(s, m):
        pl.semaphore_signal(barrier, inc=1, device_id=(s, m), device_id_type=pl.DeviceIdType.MESH)

    z_peers = [((zi + k) % ZS, ((zi + k) % ZS) * YS + yl) for k in (6, 5, 7, 4, 8, 3, 9, 2, 10, 1, 11)]
    y_peers = [((yl + k) % YS, zi * YS + (yl + k) % YS) for k in (2, 1, 3)]

    for _, m in z_peers + y_peers:
        greet(sec, m)
    for s in (ypeer, across, right, left, dpeer):
        greet(s, me)

    def pack(bufs):
        pieces = stage[...].reshape(ZS, YS, PIECE, 128)
        head = bufs[0].shape[2]
        for k in range(YS):
            bufs[0][k] = pieces[:, k, :head].astype(BF)
        bufs[4][...] = pieces[:, :, head:].astype(BF)

    started = []

    def post(src, dst, sems, i, m):
        copy = remote(src, dst, sems.at[i], sems.at[i + 1], sec, m)
        copy.start()
        return copy

    def all_of(src, dst, sems, i, count):
        copy = remote(
            src.at[pl.ds(0, count)], dst.at[pl.ds(0, count)], sems.at[i], sems.at[i + 1], sec,
            y_peers[0][1],
        )
        started.append(copy)
        return copy

    def spread(src, dst, own_index, peers, sems, i):
        for k, m in peers:
            post(src.at[k], dst.at[own_index], sems, i, m)
        dst[own_index] = src[own_index]

    def added(pieces):
        return jnp.sum(pieces[...].astype(F32), axis=0)

    def reduce_first(bufs, sems):
        spread(bufs[0], bufs[1], yl, y_peers, sems, 0)
        spread(bufs[4], bufs[5], zi, z_peers, sems, 4)

    def reduce_turn(bufs, sems):
        all_of(bufs[0], bufs[1], sems, 0, YS - 1).wait_recv()
        bufs[2][...] = added(bufs[1]).astype(BF)
        spread(bufs[2], bufs[3], zi, z_peers, sems, 2)
        all_of(bufs[4], bufs[5], sems, 4, ZS - 1).wait_recv()
        bufs[6][...] = added(bufs[5]).astype(BF)
        spread(bufs[6], bufs[7], yl, y_peers, sems, 6)

    def reduce_last(bufs, sems):
        all_of(bufs[2], bufs[3], sems, 2, ZS - 1).wait_recv()
        own[: bufs[3].shape[1]] = added(bufs[3])
        all_of(bufs[6], bufs[7], sems, 6, YS - 1).wait_recv()
        own[bufs[3].shape[1] :] = added(bufs[7])

    loads[0].wait()
    normed = norm_rows(x_v[...], ig_ref[...]).astype(BF)
    values = x_v[...].astype(F32)
    for c in range(CHUNKS):
        wide[c] = values[:, c * 128 : (c + 1) * 128]
    for c in range(CHUNKS):
        for r in range(SHARE):
            res[pl.ds(r * CHUNKS + c, 1), :] = wide[c, pl.ds(SHARE * me + r, 1), :]
    loads[1].wait()
    hidden = jnp.maximum(dot(normed, we_v[...]), 0.0).astype(BF)
    loads[2].wait()
    part = dot(hidden, wr_v[...])
    for c in range(CHUNKS):
        wide[c] = part[:, c * 128 : (c + 1) * 128]
    for c in range(CHUNKS):
        for r in range(SHARE):
            stage[pl.ds(r * CHUNKS + c, MP, stride=PIECE), :] = wide[c, pl.ds(r, MP, stride=SHARE), :]
    pack(bufs1)

    loads[3].wait()
    dec = norm_rows(dec_v[...], qg_ref[...]).astype(BF)
    loads[4].wait()
    tokens = pl.ds(pl.multiple_of(sec * QROWS, QROWS), QROWS)
    qg[tokens, 0:WIDTH] = dot(dec, wq_v[...]).astype(BF)
    loads[5].wait()
    loads[6].wait()
    qg[tokens, WIDTH : 2 * WIDTH] = dot_t(og_v[...], mix_v[...]).astype(BF)

    pl.semaphore_wait(barrier, len(z_peers) + len(y_peers) + 5)

    def rows_of(s, half=None):
        if half is None:
            return qg.at[pl.ds(pl.multiple_of(s * QROWS, QROWS), QROWS), :]
        return qg.at[pl.ds(pl.multiple_of(s * QROWS + half * (QROWS // 2), QROWS // 2), QROWS // 2), :]

    copies = []

    def forward(s, half, sems, i, to):
        ref = rows_of(s, half)
        copy = remote(ref, ref, sems[0].at[i], sems[1].at[i], to, me)
        copy.start()
        copies.append(copy)

    def arrival(s, half, sems, i):
        ref = rows_of(s, half)
        remote(ref, ref, sems[0].at[i], sems[1].at[i], dpeer, me).wait_recv()

    ys, xs, ds = (y_s, y_r), (x_s, x_r), (d_s, d_r)

    def along_x(s, half, i):
        for k, to in enumerate((right, left, across)):
            forward(s, half, xs, 3 * i + k, to)

    reduce_first(bufs1, rs_sems)
    forward(sec, 0, ys, 0, ypeer)
    along_x(sec, None, 0)
    forward(sec, None, ds, 0, dpeer)

    reduce_turn(bufs1, rs_sems)
    forward(sec, 1, ys, 1, ypeer)
    reduce_last(bufs1, rs_sems)
    rows = (own[...] + res[...]).reshape(SHARE, CHUNKS, 128)
    mean = jnp.sum(jnp.sum(rows * rows, axis=2, keepdims=True), axis=1, keepdims=True) * (1.0 / D)
    rows = rows * lax.rsqrt(mean + 1e-06) * fg_ref[...].reshape(1, CHUNKS, 128)
    own[...] = rows.reshape(PIECE, 128)
    gath_a[yl, zi] = own[:HEAD].astype(BF)
    gath_b[zi, yl] = own[HEAD:].astype(BF)
    for _, m in y_peers:
        post(gath_b.at[zi, yl], gath_b.at[zi, yl], ag_sems, 4, m)
    for _, m in z_peers:
        post(gath_a.at[yl, zi], gath_a.at[yl, zi], ag_sems, 0, m)
    for r in range(SHARE):
        for c in range(CHUNKS):
            mem_out[r : r + 1, c * 128 : (c + 1) * 128] = own[
                r * CHUNKS + c : r * CHUNKS + c + 1, :
            ].astype(BF)

    arrival(ypeer, 0, ys, 0)
    along_x(ypeer, 0, 1)
    forward(ypeer, 0, ds, 4, dpeer)
    all_of(gath_b.at[zi], gath_b.at[zi], ag_sems, 4, YS - 1).wait_recv()
    for _, m in z_peers:
        post(gath_b.at[zi], gath_b.at[zi], ag_sems, 6, m)
    near = ((section_of(3, 0, 0), 0), (section_of(1, 0, 0), 1), (section_of(2, 0, 0), 2))
    far = ((section_of(3, 1, 0), 0), (section_of(1, 1, 0), 1), (section_of(2, 1, 0), 2))
    all_of(gath_a.at[yl], gath_a.at[yl], ag_sems, 0, ZS - 1).wait_recv()
    for _, m in y_peers:
        post(gath_a.at[yl], gath_a.at[yl], ag_sems, 2, m)
    for s, k in near:
        arrival(s, None, xs, k)
        forward(s, None, ds, 1 + k, dpeer)
    arrival(ypeer, 1, ys, 1)
    along_x(ypeer, 1, 2)
    forward(ypeer, 1, ds, 5, dpeer)

    all_of(gath_b, gath_b, ag_sems, 6, ZS - 1).wait_recv()
    all_of(gath_a, gath_a, ag_sems, 2, YS - 1).wait_recv()
    for z in range(ZS):
        for y in range(YS):
            at = (z * YS + y) * PIECE
            stage[at : at + HEAD] = gath_a[y, z].astype(F32)
            stage[at + HEAD : at + PIECE] = gath_b[z, y].astype(F32)
    for r in range(SHARE):
        for c in range(CHUNKS):
            mem[r * MP : (r + 1) * MP, c * 128 : (c + 1) * 128] = stage[
                pl.ds(r * CHUNKS + c, MP, stride=PIECE), :
            ].astype(BF)
    loads[7].wait()
    keys = dot(mem[...], wk_v[...]).astype(BF)
    loads[8].wait()
    vals = dot(mem[...], wv_v[...]).astype(BF)

    def block(b):
        at = pl.ds(pl.multiple_of(b * BLOCK, BLOCK), BLOCK)
        row = pl.ds(b, 1)
        for h in range(2):
            s = dot_t(keys[:, h * DK : (h + 1) * DK], qg[at, h * DK : (h + 1) * DK]) * SCALE
            pg = dot_t(
                vals[:, h * DK : (h + 1) * DK], qg[at, WIDTH + h * DK : WIDTH + (h + 1) * DK]
            )
            top = jnp.max(s, axis=0, keepdims=True)
            w = jnp.exp(s - top)
            wts[h, b] = w
            pgr[h, b] = pg
            stats[h, 0, row, :] = top
            stats[h, 1, row, :] = jnp.sum(w, axis=0, keepdims=True)
            stats[h, 2, row, :] = jnp.sum(w * pg, axis=0, keepdims=True)

    arrival(section_of(0, 0, 1), None, ds, 0)
    block(sec // 2)
    for k, dx in enumerate((3, 1, 2)):
        arrival(section_of(dx, 0, 1), None, ds, 1 + k)
        block(section_of(dx, 0, 0) // 2)
    for half in range(2):
        for s, k in far:
            arrival(s, half, xs, 3 * (half + 1) + k)
            forward(s, half, ds, 6 + 3 * half + k, dpeer)
    for half in range(2):
        arrival(section_of(0, 1, 1), half, ds, 4 + half)
    block(ypeer // 2)
    for k, dx in enumerate((3, 1, 2)):
        for half in range(2):
            arrival(section_of(dx, 1, 1), half, ds, 6 + 3 * half + k)
        block(section_of(dx, 1, 0) // 2)

    def three(ref):
        return ref[0], ref[1], ref[2]

    def put(ref, values):
        for i in range(3):
            ref[i] = values[i]

    sd = remote(stats.at[1 - core], got_d, sd_s, sd_r, dpeer, me)
    sd.start()
    sd.wait_recv()
    put(mid, merge(three(stats.at[core]), three(got_d)))
    sy = remote(mid, got_y, sy_s, sy_r, ypeer, me)
    sy.start()
    sy.wait_recv()
    put(pair, merge(three(mid), three(got_y)))
    sx = [
        remote(pair, got_x.at[i], sx_s.at[i], sx_r.at[i], to, me)
        for i, to in enumerate((across, right, left))
    ]
    for copy in sx:
        copy.start()
    sx[1].wait_recv()
    total = merge(three(pair), three(got_x.at[1]))
    sx[2].wait_recv()
    total = merge(total, three(got_x.at[2]))
    sx[0].wait_recv()
    put(fin.at[core], merge(total, three(got_x.at[0])))
    sf = remote(fin.at[core], fin.at[core], sf_s, sf_r, dpeer, me)
    sf.start()

    def gradients(h):
        lanes = pl.ds(pl.multiple_of(h * DK, DK), DK)
        grad_lanes = pl.ds(pl.multiple_of(WIDTH + h * DK, DK), DK)

        def one(b, carry):
            at = pl.ds(pl.multiple_of(b * BLOCK, BLOCK), BLOCK)
            row = pl.ds(b, 1)
            total = fin[h, 1, row, :]
            factor = jnp.exp(stats[h, 0, row, :] - fin[h, 0, row, :]) / total
            delta = fin[h, 2, row, :] / total
            probs = wts[h, b] * factor
            sg = (probs * (pgr[h, b] - delta) * SCALE).astype(BF)
            kg = carry[0] + dot(sg, qg[at, lanes])
            vg = carry[1] + dot(probs.astype(BF), qg[at, grad_lanes])
            return kg, vg

        zero = jnp.zeros((ROWS, DK), F32)
        kg, vg = lax.fori_loop(0, BLOCKS, one, (zero, zero), unroll=2)
        grads[0, :, lanes] = kg.astype(BF)
        grads[1, :, lanes] = vg.astype(BF)

    gradients(core)
    sf.wait_recv()
    gradients(1 - core)
    part = dot_t(grads[0], wk_v[...]) + dot_t(grads[1], wv_v[...])
    for r in range(SHARE):
        for c in range(CHUNKS):
            stage[pl.ds(r * CHUNKS + c, MP, stride=PIECE), :] = part[
                r * MP : (r + 1) * MP, c * 128 : (c + 1) * 128
            ]
    pack(bufs2)
    reduce_first(bufs2, rs2_sems)
    reduce_turn(bufs2, rs2_sems)
    reduce_last(bufs2, rs2_sems)

    for copy in started + copies + [sd, sy, sf] + sx:
        copy.wait_send()
    for r in range(SHARE):
        for c in range(CHUNKS):
            grad_out[r : r + 1, c * 128 : (c + 1) * 128] = own[
                r * CHUNKS + c : r * CHUNKS + c + 1, :
            ].astype(BF)


def body(
    encoder_input, input_gain, expand_weight, reduce_weight, final_gain, decoder_input, query_gain,
    query_weight, key_weight, value_weight, mixing_weight, output_gradient,
):
    vmem = pl.BlockSpec(memory_space=pltpu.VMEM)
    hbm = pl.BlockSpec(memory_space=pl.ANY)
    dma = pltpu.SemaphoreType.DMA
    piece3 = (3, BLOCKS, BLOCK)

    def sums_at_owner(head):
        tail = PIECE - head
        shapes = (
            (YS, ZS, head, 128), (YS, ZS, head, 128), (ZS, head, 128), (ZS, head, 128),
            (ZS, YS, tail, 128), (ZS, YS, tail, 128), (YS, tail, 128), (YS, tail, 128),
        )
        return [pltpu.VMEM(shape, BF) for shape in shapes]

    out = jax.ShapeDtypeStruct((SHARE, D), BF)
    return pl.pallas_call(
        kernel,
        out_shape=(out, out),
        in_specs=[hbm, vmem, hbm, hbm, vmem, hbm, vmem, hbm, hbm, hbm, hbm, hbm],
        out_specs=(vmem, vmem),
        scratch_shapes=[
            pltpu.VMEM(encoder_input.shape, BF),
            pltpu.VMEM(expand_weight.shape, BF),
            pltpu.VMEM(reduce_weight.shape, BF),
            pltpu.VMEM(decoder_input.shape, BF),
            pltpu.VMEM(query_weight.shape, BF),
            pltpu.VMEM(key_weight.shape, BF),
            pltpu.VMEM(value_weight.shape, BF),
            pltpu.VMEM(mixing_weight.shape, BF),
            pltpu.VMEM(output_gradient.shape, BF),
            dma((9,)),
            pltpu.VMEM((CHUNKS, ROWS, 128), F32),
            pltpu.VMEM((MP * PIECE, 128), F32),
            pltpu.VMEM((PIECE, 128), F32),
            pltpu.VMEM((PIECE, 128), F32),
            sums_at_owner(1 * CHUNKS),
            sums_at_owner(2 * CHUNKS),
            pltpu.VMEM((YS, ZS, HEAD, 128), BF),
            pltpu.VMEM((ZS, YS, TAIL, 128), BF),
            pltpu.VMEM((ROWS, D), BF),
            pltpu.VMEM((QALL, 2 * WIDTH), BF),
            pltpu.VMEM((2, BLOCKS, ROWS, BLOCK), F32),
            pltpu.VMEM((2, BLOCKS, ROWS, BLOCK), F32),
            pltpu.VMEM((2, *piece3), F32),
            pltpu.VMEM(piece3, F32),
            pltpu.VMEM(piece3, F32),
            pltpu.VMEM(piece3, F32),
            pltpu.VMEM(piece3, F32),
            pltpu.VMEM((3, *piece3), F32),
            pltpu.VMEM((2, *piece3), F32),
            pltpu.VMEM((2, ROWS, WIDTH), BF),
            dma((8,)), dma((8,)), dma((8,)),
            dma((2,)), dma((2,)), dma((9,)), dma((9,)), dma((12,)), dma((12,)),
            dma, dma, dma, dma, dma((3,)), dma((3,)), dma, dma,
        ],
        compiler_params=pltpu.CompilerParams(
            collective_id=0, has_side_effects=True, vmem_limit_bytes=60 * 1024 * 1024
        ),
    )(
        encoder_input, input_gain.reshape(1, D), expand_weight, reduce_weight,
        final_gain.reshape(CHUNKS, 128), decoder_input, query_gain.reshape(1, D), query_weight,
        key_weight, value_weight, mixing_weight, output_gradient,
    )


def solution(mesh):
    in_specs = (
        P("section", None), P(), P(None, "mp"), P("mp", None), P(), P("section", None), P(),
        P(None, "mp"), P(None, "mp"), P(None, "mp"), P("mp", None), P("section", None),
    )
    out_specs = (P(("section", "mp"), None), P(("section", "mp"), None))
    return jax.shard_map(body, mesh=mesh, in_specs=in_specs, out_specs=out_specs, check_vma=False)
```

```python
import jax
import jax.numpy as jnp
from jax import lax
from jax.experimental import pallas as pl
from jax.experimental.pallas import tpu as pltpu
from jax.sharding import PartitionSpec as P

DK = 128
D = 1024
CHUNKS = D // 128
ZS, YS = 12, 4
MP = ZS * YS
ROWS = 144
SHARE = ROWS // MP
PIECE = SHARE * CHUNKS
HEAD, TAIL = 2 * CHUNKS, PIECE - 2 * CHUNKS
QROWS = 256
QALL = 4096
BLOCK = 512
BLOCKS = QALL // BLOCK
WIDTH = 2 * DK
SCALE = DK ** (-0.5)
LOG2E = 1.4426950408889634
TILE = 256
BF = jnp.bfloat16
F32 = jnp.float32


def dot(a, b):
    return jnp.dot(a, b, preferred_element_type=F32)


def dot_t(a, b):
    return lax.dot_general(a, b, (((1,), (1,)), ((), ())), preferred_element_type=F32)


def norm_rows(rows, gain):
    values = rows.astype(F32)
    return values * lax.rsqrt(jnp.mean(values * values, axis=-1, keepdims=True) + 1e-06) * gain


def merge(a, b):
    top = jnp.maximum(a[0], b[0])
    left = jnp.exp2(a[0] - top)
    right = jnp.exp2(b[0] - top)
    total = left + right
    return top + jnp.log(total) * LOG2E, (a[1] * left + b[1] * right) / total


def kernel(
    x_hbm, ig_ref, we_hbm, wr_hbm, fg_ref, dec_hbm, qg_ref, wq_hbm, wk_hbm, wv_hbm, mix_hbm, og_hbm,
    outs,
    x_v, we_v, wr_v, dec_v, wq_v, wk_v, wv_v, mix_v, og_v, load_sem,
    wide, stage, own, res, bufs1, bufs2, gath_a, gath_b, mem,
    qg, wts, pgr, tops, stats, got_d, mid, got_y, pair, got_x, fin, grads,
    rs_sems, ag_sems, rs2_sems,
    qg_s, y_r, x_r, d_r, st_s, sx_s, sd_r, sy_r, sx_r, sf_r,
):
    sec = lax.axis_index("section")
    me = lax.axis_index("mp")
    xi = sec // 4
    yi = (sec // 2) % 2
    core = sec % 2
    zi, yl = me // YS, me % YS

    def section_of(dx, dy, dc):
        return (((xi + dx) % 4) * 2 + (yi + dy) % 2) * 2 + (core + dc) % 2

    ypeer, dpeer = section_of(0, 1, 0), section_of(0, 0, 1)
    right, left, across = section_of(1, 0, 0), section_of(3, 0, 0), section_of(2, 0, 0)

    def remote(src, dst, ss, rs, s, m):
        return pltpu.make_async_remote_copy(
            src_ref=src, dst_ref=dst, send_sem=ss, recv_sem=rs, device_id=(s, m),
            device_id_type=pl.DeviceIdType.MESH,
        )

    def load(a, b, i):
        copy = pltpu.make_async_copy(a, b, load_sem.at[i])
        copy.start()
        return copy

    def load_quarters(a, b, i):
        rows = a.shape[0] // 4
        for k in range(4):
            load(a.at[pl.ds(k * rows, rows)], b.at[pl.ds(k * rows, rows)], i)
        return pltpu.make_async_copy(a, b, load_sem.at[i])

    x_load = load(x_hbm, x_v, 0)
    we_load = load_quarters(we_hbm, we_v, 1)
    wr_load = load_quarters(wr_hbm, wr_v, 2)

    barrier = pltpu.get_barrier_semaphore()

    def greet(s, m):
        pl.semaphore_signal(barrier, inc=1, device_id=(s, m), device_id_type=pl.DeviceIdType.MESH)

    z_peers = [((zi + k) % ZS, ((zi + k) % ZS) * YS + yl) for k in (6, 5, 7, 4, 8, 3, 9, 2, 10, 1, 11)]
    y_peers = [((yl + k) % YS, zi * YS + (yl + k) % YS) for k in (2, 1, 3)]

    for _, m in z_peers + y_peers:
        greet(sec, m)
    for s in (ypeer, across, right, left, dpeer):
        greet(s, me)

    def pack_y(bufs):
        pieces = stage[...].reshape(ZS, YS, PIECE, 128)
        for k in range(YS):
            bufs[0][k] = pieces[:, k, : bufs[0].shape[2]].astype(BF)

    def pack_z(bufs):
        pieces = stage[...].reshape(ZS, YS, PIECE, 128)
        bufs[4][...] = pieces[:, :, bufs[0].shape[2] :].astype(BF)

    started = []

    def post(src, dst, sems, i, m):
        copy = remote(src, dst, sems.at[i], sems.at[i + 1], sec, m)
        copy.start()
        return copy

    def all_of(src, dst, sems, i, count):
        copy = remote(
            src.at[pl.ds(0, count)], dst.at[pl.ds(0, count)], sems.at[i], sems.at[i + 1], sec,
            y_peers[0][1],
        )
        started.append(copy)
        return copy

    def spread(src, dst, own_index, peers, sems, i):
        for k, m in peers:
            post(src.at[k], dst.at[own_index], sems, i, m)
        dst[own_index] = src[own_index]

    def added(pieces):
        return jnp.sum(pieces[...].astype(F32), axis=0)

    def reduce_turn(bufs, sems):
        all_of(bufs[0], bufs[1], sems, 0, YS - 1).wait_recv()
        bufs[2][...] = added(bufs[1]).astype(BF)
        spread(bufs[2], bufs[3], zi, z_peers, sems, 2)
        all_of(bufs[4], bufs[5], sems, 4, ZS - 1).wait_recv()
        bufs[6][...] = added(bufs[5]).astype(BF)
        spread(bufs[6], bufs[7], yl, y_peers, sems, 6)

    def reduce_last(bufs, sems):
        all_of(bufs[2], bufs[3], sems, 2, ZS - 1).wait_recv()
        own[: bufs[3].shape[1]] = added(bufs[3])
        all_of(bufs[6], bufs[7], sems, 6, YS - 1).wait_recv()
        own[bufs[3].shape[1] :] = added(bufs[7])

    x_load.wait()
    normed = norm_rows(x_v[...], ig_ref[...]).astype(BF)
    values = x_v[...].astype(F32)
    for c in range(CHUNKS):
        wide[c] = values[:, c * 128 : (c + 1) * 128]
    for c in range(CHUNKS):
        for r in range(SHARE):
            res[pl.ds(r * CHUNKS + c, 1), :] = wide[c, pl.ds(SHARE * me + r, 1), :]
    we_load.wait()
    loads = [
        load(a, b, 3 + i)
        for i, (a, b) in enumerate(
            (
                (dec_hbm, dec_v), (wq_hbm, wq_v), (og_hbm, og_v), (mix_hbm, mix_v), (wk_hbm, wk_v),
                (wv_hbm, wv_v),
            )
        )
    ]
    hidden = jnp.maximum(dot(normed, we_v[...]), 0.0).astype(BF)
    wr_load.wait()
    part = dot(hidden, wr_v[...])
    for c in range(CHUNKS):
        wide[c] = part[:, c * 128 : (c + 1) * 128]
    for c in range(CHUNKS):
        for r in range(SHARE):
            stage[pl.ds(r * CHUNKS + c, MP, stride=PIECE), :] = wide[c, pl.ds(r, MP, stride=SHARE), :]
    pack_y(bufs1)
    pack_z(bufs1)

    loads[0].wait()
    dec = norm_rows(dec_v[...], qg_ref[...]).astype(BF)
    loads[1].wait()
    tokens = pl.ds(pl.multiple_of(sec * QROWS, QROWS), QROWS)
    qg[tokens, 0:WIDTH] = dot(dec, wq_v[...]).astype(BF)
    loads[2].wait()
    loads[3].wait()
    qg[tokens, WIDTH : 2 * WIDTH] = dot_t(og_v[...], mix_v[...]).astype(BF)

    pl.semaphore_wait(barrier, len(z_peers) + len(y_peers) + 5)

    parts = ((0, QROWS // 2), (QROWS // 2, QROWS // 4), (3 * QROWS // 4, QROWS // 4))

    def rows_of(s, part=None):
        first, count = (0, QROWS) if part is None else parts[part]
        return qg.at[pl.ds(pl.multiple_of(s * QROWS + first, QROWS // 4), count), :]

    def forward(s, part, recv_sem, to):
        ref = rows_of(s, part)
        remote(ref, ref, qg_s, recv_sem, to, me).start()

    def arrived(count, recv_sem):
        ref = qg.at[pl.ds(0, count), :]
        remote(ref, ref, qg_s, recv_sem, dpeer, me).wait_recv()

    def along_x(s, part, i):
        for to in (right, left, across):
            forward(s, part, x_r.at[i], to)

    spread(bufs1[0], bufs1[1], yl, y_peers, rs_sems, 0)
    spread(bufs1[4], bufs1[5], zi, z_peers, rs_sems, 4)
    forward(sec, 0, y_r.at[0], ypeer)
    along_x(sec, None, 0)
    forward(sec, None, d_r.at[0], dpeer)

    reduce_turn(bufs1, rs_sems)
    forward(sec, 1, y_r.at[1], ypeer)
    arrived(parts[0][1], y_r.at[0])
    along_x(ypeer, 0, 1)
    forward(ypeer, 0, d_r.at[1], dpeer)
    reduce_last(bufs1, rs_sems)
    rows = (own[...] + res[...]).reshape(SHARE, CHUNKS, 128)
    mean = jnp.sum(jnp.sum(rows * rows, axis=2, keepdims=True), axis=1, keepdims=True) * (1.0 / D)
    rows = rows * lax.rsqrt(mean + 1e-06) * fg_ref[...].reshape(1, CHUNKS, 128)
    own[...] = rows.reshape(PIECE, 128)
    gath_a[yl, zi] = own[:HEAD].astype(BF)
    gath_b[zi, yl] = own[HEAD:].astype(BF)
    for _, m in y_peers:
        post(gath_b.at[zi, yl], gath_b.at[zi, yl], ag_sems, 4, m)
    for _, m in z_peers:
        post(gath_a.at[yl, zi], gath_a.at[yl, zi], ag_sems, 0, m)
    forward(sec, 2, y_r.at[2], ypeer)
    for r in range(SHARE):
        for c in range(CHUNKS):
            outs[0, r : r + 1, c * 128 : (c + 1) * 128] = own[
                r * CHUNKS + c : r * CHUNKS + c + 1, :
            ].astype(BF)

    all_of(gath_b.at[zi], gath_b.at[zi], ag_sems, 4, YS - 1).wait_recv()
    for _, m in z_peers:
        post(gath_b.at[zi], gath_b.at[zi], ag_sems, 6, m)
    arrived(parts[1][1], y_r.at[1])
    along_x(ypeer, 1, 2)
    forward(ypeer, 1, d_r.at[1], dpeer)
    def far_on(part):
        arrived(3 * parts[part][1], x_r.at[part + 1])
        for dx in (3, 1, 2):
            forward(section_of(dx, 1, 0), part, d_r.at[1], dpeer)

    all_of(gath_a.at[yl], gath_a.at[yl], ag_sems, 0, ZS - 1).wait_recv()
    for _, m in y_peers:
        post(gath_a.at[yl], gath_a.at[yl], ag_sems, 2, m)
    arrived(3 * QROWS, x_r.at[0])
    for dx in (3, 1, 2):
        forward(section_of(dx, 0, 0), None, d_r.at[0], dpeer)
    arrived(parts[2][1], y_r.at[2])
    along_x(ypeer, 2, 3)
    forward(ypeer, 2, d_r.at[1], dpeer)

    far_on(0)

    def memory_rows(r, piece, line):
        for z in range(ZS):
            for y in range(YS):
                at = (z * YS + y) * PIECE + r * CHUNKS
                stage[at : at + CHUNKS] = piece(z, y)[line : line + CHUNKS].astype(F32)
        for c in range(CHUNKS):
            mem[r * MP : (r + 1) * MP, c * 128 : (c + 1) * 128] = stage[
                pl.ds(r * CHUNKS + c, MP, stride=PIECE), :
            ].astype(BF)

    all_of(gath_b, gath_b, ag_sems, 6, ZS - 1).wait_recv()
    memory_rows(2, lambda z, y: gath_b[z, y], 0)
    all_of(gath_a, gath_a, ag_sems, 2, YS - 1).wait_recv()
    for r in range(2):
        memory_rows(r, lambda z, y: gath_a[y, z], r * CHUNKS)
    loads[4].wait()
    keys = dot(mem[...], wk_v[...]).astype(BF)
    loads[5].wait()
    vals = dot(mem[...], wv_v[...]).astype(BF)

    def block(b):
        row = pl.ds(b, 1)
        for h in range(2):
            for q in range(BLOCK // TILE):
                at = pl.ds(pl.multiple_of(b * BLOCK + q * TILE, TILE), TILE)
                cols = slice(q * TILE, (q + 1) * TILE)
                s = dot_t(keys[:, h * DK : (h + 1) * DK], qg[at, h * DK : (h + 1) * DK])
                s = s * (SCALE * LOG2E)
                pg = dot_t(
                    vals[:, h * DK : (h + 1) * DK], qg[at, WIDTH + h * DK : WIDTH + (h + 1) * DK]
                )
                top = jnp.max(s, axis=0, keepdims=True)
                w = jnp.exp2(s - top)
                wts[h, b, :, cols] = w
                pgr[h, b, :, cols] = pg
                total = jnp.sum(w, axis=0, keepdims=True)
                tops[h, row, cols] = top
                stats[h, 0, row, cols] = top + jnp.log(total) * LOG2E
                stats[h, 1, row, cols] = jnp.sum(w * pg, axis=0, keepdims=True) / total

    far_on(1)
    far_on(2)
    arrived(4 * QROWS, d_r.at[0])
    for dx in (0, 3, 1, 2):
        block(section_of(dx, 0, 0) // 2)
    arrived(4 * QROWS, d_r.at[1])
    for dx in (0, 3, 1, 2):
        block(section_of(dx, 1, 0) // 2)

    def both(ref):
        return ref[0], ref[1]

    def put(ref, values):
        for i in range(2):
            ref[i] = values[i]

    sd = remote(stats.at[1 - core], got_d, st_s, sd_r, dpeer, me)
    sd.start()
    sd.wait_recv()
    put(mid, merge(both(stats.at[core]), both(got_d)))
    sy = remote(mid, got_y, st_s, sy_r, ypeer, me)
    sy.start()
    sy.wait_recv()
    put(pair, merge(both(mid), both(got_y)))
    for i, to in enumerate((across, right, left)):
        remote(pair, got_x.at[i], sx_s, sx_r, to, me).start()
    sx = remote(got_x, got_x, sx_s, sx_r, across, me)
    sx.wait_recv()
    total = merge(both(pair), both(got_x.at[1]))
    total = merge(total, both(got_x.at[2]))
    put(fin.at[core], merge(total, both(got_x.at[0])))
    sf = remote(fin.at[core], fin.at[core], st_s, sf_r, dpeer, me)
    sf.start()

    def gradients(h):
        lanes = pl.ds(pl.multiple_of(h * DK, DK), DK)
        grad_lanes = pl.ds(pl.multiple_of(WIDTH + h * DK, DK), DK)

        def one(b, carry):
            at = pl.ds(pl.multiple_of(b * BLOCK, BLOCK), BLOCK)
            row = pl.ds(b, 1)
            factor = jnp.exp2(tops[h, row, :] - fin[h, 0, row, :])
            delta = fin[h, 1, row, :]
            probs = wts[h, b] * factor
            sg = (probs * (pgr[h, b] - delta) * SCALE).astype(BF)
            kg = carry[0] + dot(sg, qg[at, lanes])
            vg = carry[1] + dot(probs.astype(BF), qg[at, grad_lanes])
            return kg, vg

        zero = jnp.zeros((ROWS, DK), F32)
        kg, vg = lax.fori_loop(0, BLOCKS, one, (zero, zero), unroll=True)
        grads[0, :, lanes] = kg.astype(BF)
        grads[1, :, lanes] = vg.astype(BF)

    gradients(core)
    sf.wait_recv()
    gradients(1 - core)
    def partial_rows(first, last):
        low, high = first * MP, last * MP
        part = dot_t(grads[0, low:high], wk_v[...]) + dot_t(grads[1, low:high], wv_v[...])
        for r in range(first, last):
            for c in range(CHUNKS):
                stage[pl.ds(r * CHUNKS + c, MP, stride=PIECE), :] = part[
                    (r - first) * MP : (r - first + 1) * MP, c * 128 : (c + 1) * 128
                ]

    partial_rows(0, 2)
    pack_y(bufs2)
    spread(bufs2[0], bufs2[1], yl, y_peers, rs2_sems, 0)
    partial_rows(2, 3)
    pack_z(bufs2)
    spread(bufs2[4], bufs2[5], zi, z_peers, rs2_sems, 4)
    reduce_turn(bufs2, rs2_sems)
    reduce_last(bufs2, rs2_sems)

    for copy in started:
        copy.wait_send()
    sent = qg.at[pl.ds(0, 15 * QROWS), :]
    remote(sent, sent, qg_s, d_r.at[0], dpeer, me).wait_send()
    sx.wait_send()
    remote(got_x, got_x, st_s, sx_r, dpeer, me).wait_send()
    for r in range(SHARE):
        for c in range(CHUNKS):
            outs[1, r : r + 1, c * 128 : (c + 1) * 128] = own[
                r * CHUNKS + c : r * CHUNKS + c + 1, :
            ].astype(BF)


def body(
    encoder_input, input_gain, expand_weight, reduce_weight, final_gain, decoder_input, query_gain,
    query_weight, key_weight, value_weight, mixing_weight, output_gradient,
):
    vmem = pl.BlockSpec(memory_space=pltpu.VMEM)
    hbm = pl.BlockSpec(memory_space=pl.ANY)
    dma = pltpu.SemaphoreType.DMA
    piece2 = (2, BLOCKS, BLOCK)

    def sums_at_owner(head):
        tail = PIECE - head
        shapes = (
            (YS, ZS, head, 128), (YS, ZS, head, 128), (ZS, head, 128), (ZS, head, 128),
            (ZS, YS, tail, 128), (ZS, YS, tail, 128), (YS, tail, 128), (YS, tail, 128),
        )
        return [pltpu.VMEM(shape, BF) for shape in shapes]

    outs = pl.pallas_call(
        kernel,
        out_shape=pltpu.VMEM((2, SHARE, D), BF),
        in_specs=[hbm, vmem, hbm, hbm, vmem, hbm, vmem, hbm, hbm, hbm, hbm, hbm],
        out_specs=vmem,
        scratch_shapes=[
            pltpu.VMEM(encoder_input.shape, BF),
            pltpu.VMEM(expand_weight.shape, BF),
            pltpu.VMEM(reduce_weight.shape, BF),
            pltpu.VMEM(decoder_input.shape, BF),
            pltpu.VMEM(query_weight.shape, BF),
            pltpu.VMEM(key_weight.shape, BF),
            pltpu.VMEM(value_weight.shape, BF),
            pltpu.VMEM(mixing_weight.shape, BF),
            pltpu.VMEM(output_gradient.shape, BF),
            dma((9,)),
            pltpu.VMEM((CHUNKS, ROWS, 128), F32),
            pltpu.VMEM((MP * PIECE, 128), F32),
            pltpu.VMEM((PIECE, 128), F32),
            pltpu.VMEM((PIECE, 128), F32),
            sums_at_owner(1 * CHUNKS),
            sums_at_owner(2 * CHUNKS),
            pltpu.VMEM((YS, ZS, HEAD, 128), BF),
            pltpu.VMEM((ZS, YS, TAIL, 128), BF),
            pltpu.VMEM((ROWS, D), BF),
            pltpu.VMEM((QALL, 2 * WIDTH), BF),
            pltpu.VMEM((2, BLOCKS, ROWS, BLOCK), F32),
            pltpu.VMEM((2, BLOCKS, ROWS, BLOCK), F32),
            pltpu.VMEM((2, BLOCKS, BLOCK), F32),
            pltpu.VMEM((2, *piece2), F32),
            pltpu.VMEM(piece2, F32),
            pltpu.VMEM(piece2, F32),
            pltpu.VMEM(piece2, F32),
            pltpu.VMEM(piece2, F32),
            pltpu.VMEM((3, *piece2), F32),
            pltpu.VMEM((2, *piece2), F32),
            pltpu.VMEM((2, ROWS, WIDTH), BF),
            dma((8,)), dma((8,)), dma((8,)),
            dma, dma((3,)), dma((4,)), dma((2,)), dma, dma, dma, dma, dma, dma,
        ],
        compiler_params=pltpu.CompilerParams(
            collective_id=0, has_side_effects=True, vmem_limit_bytes=60 * 1024 * 1024
        ),
    )(
        encoder_input, input_gain.reshape(1, D), expand_weight, reduce_weight,
        final_gain.reshape(CHUNKS, 128), decoder_input, query_gain.reshape(1, D), query_weight,
        key_weight, value_weight, mixing_weight, output_gradient,
    )
    return outs[0], outs[1]


def solution(mesh):
    in_specs = (
        P("section", None), P(), P(None, "mp"), P("mp", None), P(), P("section", None), P(),
        P(None, "mp"), P(None, "mp"), P(None, "mp"), P("mp", None), P("section", None),
    )
    out_specs = (P(("section", "mp"), None), P(("section", "mp"), None))
    return jax.shard_map(body, mesh=mesh, in_specs=in_specs, out_specs=out_specs, check_vma=False)
```

```python
import jax
import jax.numpy as jnp
from jax import lax
from jax.experimental import pallas as pl
from jax.experimental.pallas import tpu as pltpu
from jax.sharding import PartitionSpec as P

DK = 128
D = 1024
CHUNKS = D // 128
ZS, YS = 12, 4
MP = ZS * YS
ROWS = 144
SHARE = ROWS // MP
PIECE = SHARE * CHUNKS
HEAD, TAIL = 2 * CHUNKS, PIECE - 2 * CHUNKS
QROWS = 256
QALL = 4096
BLOCK = 512
BLOCKS = QALL // BLOCK
WIDTH = 2 * DK
SCALE = DK ** (-0.5)
LOG2E = 1.4426950408889634
TILE = 256
BF = jnp.bfloat16
F32 = jnp.float32


def dot(a, b):
    return jnp.dot(a, b, preferred_element_type=F32)


def dot_t(a, b):
    return lax.dot_general(a, b, (((1,), (1,)), ((), ())), preferred_element_type=F32)


def norm_rows(rows, gain):
    values = rows.astype(F32)
    return values * lax.rsqrt(jnp.mean(values * values, axis=-1, keepdims=True) + 1e-06) * gain


def merge(a, b):
    top = jnp.maximum(a[0], b[0])
    left = jnp.exp2(a[0] - top)
    right = jnp.exp2(b[0] - top)
    total = left + right
    return top + jnp.log(total) * LOG2E, (a[1] * left + b[1] * right) / total


def kernel(
    x_hbm, ig_ref, we_hbm, wr_hbm, fg_ref, dec_hbm, qg_ref, wq_hbm, wk_hbm, wv_hbm, mix_hbm, og_hbm,
    outs,
    x_v, we_v, wr_v, dec_v, wq_v, wk_v, wv_v, mix_v, og_v, load_sem,
    wide, stage, own, res, bufs1, bufs2, gath_a, gath_b, mem,
    qg, wts, pgr, tops, stats, got_d, mid, got_y, pair, got_x, fin, grads,
    rs_sems, ag_sems, rs2_sems,
    qg_s, y_r, x_r, d_r, st_s, sx_s, sd_r, sy_r, sx_r, sf_r,
):
    sec = lax.axis_index("section")
    me = lax.axis_index("mp")
    xi = sec // 4
    yi = (sec // 2) % 2
    core = sec % 2
    zi, yl = me // YS, me % YS

    def section_of(dx, dy, dc):
        return (((xi + dx) % 4) * 2 + (yi + dy) % 2) * 2 + (core + dc) % 2

    ypeer, dpeer = section_of(0, 1, 0), section_of(0, 0, 1)
    right, left, across = section_of(1, 0, 0), section_of(3, 0, 0), section_of(2, 0, 0)

    def remote(src, dst, ss, rs, s, m):
        return pltpu.make_async_remote_copy(
            src_ref=src, dst_ref=dst, send_sem=ss, recv_sem=rs, device_id=(s, m),
            device_id_type=pl.DeviceIdType.MESH,
        )

    def load(a, b, i):
        copy = pltpu.make_async_copy(a, b, load_sem.at[i])
        copy.start()
        return copy

    def load_quarters(a, b, i):
        rows = a.shape[0] // 4
        for k in range(4):
            load(a.at[pl.ds(k * rows, rows)], b.at[pl.ds(k * rows, rows)], i)
        return pltpu.make_async_copy(a, b, load_sem.at[i])

    x_load = load(x_hbm, x_v, 0)
    we_load = load_quarters(we_hbm, we_v, 1)
    wr_load = load_quarters(wr_hbm, wr_v, 2)

    barrier = pltpu.get_barrier_semaphore()

    def greet(s, m):
        pl.semaphore_signal(barrier, inc=1, device_id=(s, m), device_id_type=pl.DeviceIdType.MESH)

    z_peers = [((zi + k) % ZS, ((zi + k) % ZS) * YS + yl) for k in (6, 5, 7, 4, 8, 3, 9, 2, 10, 1, 11)]
    y_peers = [((yl + k) % YS, zi * YS + (yl + k) % YS) for k in (2, 1, 3)]

    for _, m in z_peers + y_peers:
        greet(sec, m)
    for s in (ypeer, across, right, left, dpeer):
        greet(s, me)

    def pack_y(bufs):
        pieces = stage[...].reshape(ZS, YS, PIECE, 128)
        for k in range(YS):
            bufs[0][k] = pieces[:, k, : bufs[0].shape[2]].astype(BF)

    def pack_z(bufs):
        pieces = stage[...].reshape(ZS, YS, PIECE, 128)
        bufs[4][...] = pieces[:, :, bufs[0].shape[2] :].astype(BF)

    started = []

    def post(src, dst, sems, i, m):
        copy = remote(src, dst, sems.at[i], sems.at[i + 1], sec, m)
        copy.start()
        return copy

    def all_of(src, dst, sems, i, count):
        copy = remote(
            src.at[pl.ds(0, count)], dst.at[pl.ds(0, count)], sems.at[i], sems.at[i + 1], sec,
            y_peers[0][1],
        )
        started.append(copy)
        return copy

    def spread(src, dst, own_index, peers, sems, i):
        for k, m in peers:
            post(src.at[k], dst.at[own_index], sems, i, m)
        dst[own_index] = src[own_index]

    def added(pieces):
        return jnp.sum(pieces[...].astype(F32), axis=0)

    def reduce_turn(bufs, sems):
        all_of(bufs[0], bufs[1], sems, 0, YS - 1).wait_recv()
        bufs[2][...] = added(bufs[1]).astype(BF)
        spread(bufs[2], bufs[3], zi, z_peers, sems, 2)
        all_of(bufs[4], bufs[5], sems, 4, ZS - 1).wait_recv()
        bufs[6][...] = added(bufs[5]).astype(BF)
        spread(bufs[6], bufs[7], yl, y_peers, sems, 6)

    def reduce_last(bufs, sems):
        all_of(bufs[2], bufs[3], sems, 2, ZS - 1).wait_recv()
        own[: bufs[3].shape[1]] = added(bufs[3])
        all_of(bufs[6], bufs[7], sems, 6, YS - 1).wait_recv()
        own[bufs[3].shape[1] :] = added(bufs[7])

    x_load.wait()
    normed = norm_rows(x_v[...], ig_ref[...]).astype(BF)
    values = x_v[...].astype(F32)
    for c in range(CHUNKS):
        wide[c] = values[:, c * 128 : (c + 1) * 128]
    for c in range(CHUNKS):
        for r in range(SHARE):
            res[pl.ds(r * CHUNKS + c, 1), :] = wide[c, pl.ds(SHARE * me + r, 1), :]
    we_load.wait()
    loads = [
        load(a, b, 3 + i)
        for i, (a, b) in enumerate(
            (
                (dec_hbm, dec_v), (wq_hbm, wq_v), (og_hbm, og_v), (mix_hbm, mix_v), (wk_hbm, wk_v),
                (wv_hbm, wv_v),
            )
        )
    ]
    hidden = jnp.maximum(dot(normed, we_v[...]), 0.0).astype(BF)
    wr_load.wait()
    part = dot(hidden, wr_v[...])
    for c in range(CHUNKS):
        wide[c] = part[:, c * 128 : (c + 1) * 128]
    for c in range(CHUNKS):
        for r in range(SHARE):
            stage[pl.ds(r * CHUNKS + c, MP, stride=PIECE), :] = wide[c, pl.ds(r, MP, stride=SHARE), :]
    pack_y(bufs1)
    pack_z(bufs1)

    loads[0].wait()
    dec = norm_rows(dec_v[...], qg_ref[...]).astype(BF)
    loads[1].wait()
    tokens = pl.ds(pl.multiple_of(sec * QROWS, QROWS), QROWS)
    qg[tokens, 0:WIDTH] = dot(dec, wq_v[...]).astype(BF)
    loads[2].wait()
    loads[3].wait()
    qg[tokens, WIDTH : 2 * WIDTH] = dot_t(og_v[...], mix_v[...]).astype(BF)

    pl.semaphore_wait(barrier, len(z_peers) + len(y_peers) + 5)

    parts = ((0, 112), (112, 80), (192, 64), (0, 128), (128, 128))

    def rows_of(s, part=None):
        first, count = (0, QROWS) if part is None else parts[part]
        return qg.at[pl.ds(pl.multiple_of(s * QROWS + first, 16), count), :]

    def forward(s, part, recv_sem, to):
        ref = rows_of(s, part)
        remote(ref, ref, qg_s, recv_sem, to, me).start()

    def arrived(count, recv_sem):
        ref = qg.at[pl.ds(0, count), :]
        remote(ref, ref, qg_s, recv_sem, dpeer, me).wait_recv()

    def along_x(s, part, i):
        for to in (right, left, across):
            forward(s, part, x_r.at[i], to)

    spread(bufs1[0], bufs1[1], yl, y_peers, rs_sems, 0)
    spread(bufs1[4], bufs1[5], zi, z_peers, rs_sems, 4)
    forward(sec, 0, y_r.at[0], ypeer)
    for to in (right, left):
        forward(sec, None, x_r.at[0], to)
    forward(sec, None, d_r.at[0], dpeer)

    reduce_turn(bufs1, rs_sems)
    forward(sec, 1, y_r.at[1], ypeer)
    arrived(2 * QROWS, x_r.at[0])
    forward(left, 3, x_r.at[4], right)
    forward(right, 4, x_r.at[4], left)
    for s in (left, right):
        forward(s, None, d_r.at[0], dpeer)
    arrived(parts[0][1], y_r.at[0])
    along_x(ypeer, 0, 1)
    forward(ypeer, 0, d_r.at[1], dpeer)
    reduce_last(bufs1, rs_sems)
    rows = (own[...] + res[...]).reshape(SHARE, CHUNKS, 128)
    mean = jnp.sum(jnp.sum(rows * rows, axis=2, keepdims=True), axis=1, keepdims=True) * (1.0 / D)
    rows = rows * lax.rsqrt(mean + 1e-06) * fg_ref[...].reshape(1, CHUNKS, 128)
    own[...] = rows.reshape(PIECE, 128)
    gath_a[yl, zi] = own[:HEAD].astype(BF)
    gath_b[zi, yl] = own[HEAD:].astype(BF)
    for _, m in y_peers:
        post(gath_b.at[zi, yl], gath_b.at[zi, yl], ag_sems, 4, m)
    for _, m in z_peers:
        post(gath_a.at[yl, zi], gath_a.at[yl, zi], ag_sems, 0, m)
    forward(sec, 2, y_r.at[2], ypeer)
    for r in range(SHARE):
        for c in range(CHUNKS):
            outs[0, r : r + 1, c * 128 : (c + 1) * 128] = own[
                r * CHUNKS + c : r * CHUNKS + c + 1, :
            ].astype(BF)

    all_of(gath_b.at[zi], gath_b.at[zi], ag_sems, 4, YS - 1).wait_recv()
    for _, m in z_peers:
        post(gath_b.at[zi], gath_b.at[zi], ag_sems, 6, m)
    arrived(parts[1][1], y_r.at[1])
    along_x(ypeer, 1, 2)
    forward(ypeer, 1, d_r.at[1], dpeer)
    def far_on(part):
        arrived(3 * parts[part][1], x_r.at[part + 1])
        for dx in (3, 1, 2):
            forward(section_of(dx, 1, 0), part, d_r.at[1], dpeer)

    all_of(gath_a.at[yl], gath_a.at[yl], ag_sems, 0, ZS - 1).wait_recv()
    for _, m in y_peers:
        post(gath_a.at[yl], gath_a.at[yl], ag_sems, 2, m)
    arrived(QROWS, x_r.at[4])
    forward(across, None, d_r.at[0], dpeer)
    arrived(parts[2][1], y_r.at[2])
    along_x(ypeer, 2, 3)
    forward(ypeer, 2, d_r.at[1], dpeer)

    far_on(0)

    def memory_rows(r, piece, line):
        for z in range(ZS):
            for y in range(YS):
                at = (z * YS + y) * PIECE + r * CHUNKS
                stage[at : at + CHUNKS] = piece(z, y)[line : line + CHUNKS].astype(F32)
        for c in range(CHUNKS):
            mem[r * MP : (r + 1) * MP, c * 128 : (c + 1) * 128] = stage[
                pl.ds(r * CHUNKS + c, MP, stride=PIECE), :
            ].astype(BF)

    all_of(gath_b, gath_b, ag_sems, 6, ZS - 1).wait_recv()
    memory_rows(2, lambda z, y: gath_b[z, y], 0)
    far_on(1)
    all_of(gath_a, gath_a, ag_sems, 2, YS - 1).wait_recv()
    for r in range(2):
        memory_rows(r, lambda z, y: gath_a[y, z], r * CHUNKS)
    loads[4].wait()
    keys = dot(mem[...], wk_v[...]).astype(BF)
    loads[5].wait()
    vals = dot(mem[...], wv_v[...]).astype(BF)

    def block(b):
        row = pl.ds(b, 1)
        for h in range(2):
            for q in range(BLOCK // TILE):
                at = pl.ds(pl.multiple_of(b * BLOCK + q * TILE, TILE), TILE)
                cols = slice(q * TILE, (q + 1) * TILE)
                s = dot_t(keys[:, h * DK : (h + 1) * DK], qg[at, h * DK : (h + 1) * DK])
                s = s * (SCALE * LOG2E)
                pg = dot_t(
                    vals[:, h * DK : (h + 1) * DK], qg[at, WIDTH + h * DK : WIDTH + (h + 1) * DK]
                )
                top = jnp.max(s, axis=0, keepdims=True)
                w = jnp.exp2(s - top)
                wts[h, b, :, cols] = w
                pgr[h, b, :, cols] = pg
                total = jnp.sum(w, axis=0, keepdims=True)
                tops[h, row, cols] = top
                stats[h, 0, row, cols] = top + jnp.log(total) * LOG2E
                stats[h, 1, row, cols] = jnp.sum(w * pg, axis=0, keepdims=True) / total

    far_on(2)
    arrived(4 * QROWS, d_r.at[0])
    for dx in (0, 3, 1, 2):
        block(section_of(dx, 0, 0) // 2)
    arrived(4 * QROWS, d_r.at[1])
    for dx in (0, 3, 1, 2):
        block(section_of(dx, 1, 0) // 2)

    def both(ref):
        return ref[0], ref[1]

    def put(ref, values):
        for i in range(2):
            ref[i] = values[i]

    sd = remote(stats.at[1 - core], got_d, st_s, sd_r, dpeer, me)
    sd.start()
    sd.wait_recv()
    put(mid, merge(both(stats.at[core]), both(got_d)))
    sy = remote(mid, got_y, st_s, sy_r, ypeer, me)
    sy.start()
    sy.wait_recv()
    put(pair, merge(both(mid), both(got_y)))
    for i, to in enumerate((across, right, left)):
        remote(pair, got_x.at[i], sx_s, sx_r, to, me).start()
    sx = remote(got_x, got_x, sx_s, sx_r, across, me)
    sx.wait_recv()
    total = merge(both(pair), both(got_x.at[1]))
    total = merge(total, both(got_x.at[2]))
    put(fin.at[core], merge(total, both(got_x.at[0])))
    sf = remote(fin.at[core], fin.at[core], st_s, sf_r, dpeer, me)
    sf.start()

    def gradients(h):
        lanes = pl.ds(pl.multiple_of(h * DK, DK), DK)
        grad_lanes = pl.ds(pl.multiple_of(WIDTH + h * DK, DK), DK)

        def one(b, carry):
            at = pl.ds(pl.multiple_of(b * BLOCK, BLOCK), BLOCK)
            row = pl.ds(b, 1)
            factor = jnp.exp2(tops[h, row, :] - fin[h, 0, row, :])
            delta = fin[h, 1, row, :]
            probs = wts[h, b] * factor
            sg = (probs * (pgr[h, b] - delta) * SCALE).astype(BF)
            kg = carry[0] + dot(sg, qg[at, lanes])
            vg = carry[1] + dot(probs.astype(BF), qg[at, grad_lanes])
            return kg, vg

        zero = jnp.zeros((ROWS, DK), F32)
        kg, vg = lax.fori_loop(0, BLOCKS, one, (zero, zero), unroll=True)
        grads[0, :, lanes] = kg.astype(BF)
        grads[1, :, lanes] = vg.astype(BF)

    gradients(core)
    sf.wait_recv()
    gradients(1 - core)
    def partial_rows(first, last):
        low, high = first * MP, last * MP
        part = dot_t(grads[0, low:high], wk_v[...]) + dot_t(grads[1, low:high], wv_v[...])
        for r in range(first, last):
            for c in range(CHUNKS):
                stage[pl.ds(r * CHUNKS + c, MP, stride=PIECE), :] = part[
                    (r - first) * MP : (r - first + 1) * MP, c * 128 : (c + 1) * 128
                ]

    partial_rows(0, 2)
    pack_y(bufs2)
    spread(bufs2[0], bufs2[1], yl, y_peers, rs2_sems, 0)
    partial_rows(2, 3)
    pack_z(bufs2)
    spread(bufs2[4], bufs2[5], zi, z_peers, rs2_sems, 4)
    reduce_turn(bufs2, rs2_sems)
    reduce_last(bufs2, rs2_sems)

    for copy in started:
        copy.wait_send()
    sent = qg.at[pl.ds(0, 15 * QROWS), :]
    remote(sent, sent, qg_s, d_r.at[0], dpeer, me).wait_send()
    sx.wait_send()
    remote(got_x, got_x, st_s, sx_r, dpeer, me).wait_send()
    for r in range(SHARE):
        for c in range(CHUNKS):
            outs[1, r : r + 1, c * 128 : (c + 1) * 128] = own[
                r * CHUNKS + c : r * CHUNKS + c + 1, :
            ].astype(BF)


def body(
    encoder_input, input_gain, expand_weight, reduce_weight, final_gain, decoder_input, query_gain,
    query_weight, key_weight, value_weight, mixing_weight, output_gradient,
):
    vmem = pl.BlockSpec(memory_space=pltpu.VMEM)
    hbm = pl.BlockSpec(memory_space=pl.ANY)
    dma = pltpu.SemaphoreType.DMA
    piece2 = (2, BLOCKS, BLOCK)

    def sums_at_owner(head):
        tail = PIECE - head
        shapes = (
            (YS, ZS, head, 128), (YS, ZS, head, 128), (ZS, head, 128), (ZS, head, 128),
            (ZS, YS, tail, 128), (ZS, YS, tail, 128), (YS, tail, 128), (YS, tail, 128),
        )
        return [pltpu.VMEM(shape, BF) for shape in shapes]

    outs = pl.pallas_call(
        kernel,
        out_shape=pltpu.VMEM((2, SHARE, D), BF),
        in_specs=[hbm, vmem, hbm, hbm, vmem, hbm, vmem, hbm, hbm, hbm, hbm, hbm],
        out_specs=vmem,
        scratch_shapes=[
            pltpu.VMEM(encoder_input.shape, BF),
            pltpu.VMEM(expand_weight.shape, BF),
            pltpu.VMEM(reduce_weight.shape, BF),
            pltpu.VMEM(decoder_input.shape, BF),
            pltpu.VMEM(query_weight.shape, BF),
            pltpu.VMEM(key_weight.shape, BF),
            pltpu.VMEM(value_weight.shape, BF),
            pltpu.VMEM(mixing_weight.shape, BF),
            pltpu.VMEM(output_gradient.shape, BF),
            dma((9,)),
            pltpu.VMEM((CHUNKS, ROWS, 128), F32),
            pltpu.VMEM((MP * PIECE, 128), F32),
            pltpu.VMEM((PIECE, 128), F32),
            pltpu.VMEM((PIECE, 128), F32),
            sums_at_owner(1 * CHUNKS),
            sums_at_owner(2 * CHUNKS),
            pltpu.VMEM((YS, ZS, HEAD, 128), BF),
            pltpu.VMEM((ZS, YS, TAIL, 128), BF),
            pltpu.VMEM((ROWS, D), BF),
            pltpu.VMEM((QALL, 2 * WIDTH), BF),
            pltpu.VMEM((2, BLOCKS, ROWS, BLOCK), F32),
            pltpu.VMEM((2, BLOCKS, ROWS, BLOCK), F32),
            pltpu.VMEM((2, BLOCKS, BLOCK), F32),
            pltpu.VMEM((2, *piece2), F32),
            pltpu.VMEM(piece2, F32),
            pltpu.VMEM(piece2, F32),
            pltpu.VMEM(piece2, F32),
            pltpu.VMEM(piece2, F32),
            pltpu.VMEM((3, *piece2), F32),
            pltpu.VMEM((2, *piece2), F32),
            pltpu.VMEM((2, ROWS, WIDTH), BF),
            dma((8,)), dma((8,)), dma((8,)),
            dma, dma((3,)), dma((5,)), dma((2,)), dma, dma, dma, dma, dma, dma,
        ],
        compiler_params=pltpu.CompilerParams(
            collective_id=0, has_side_effects=True, vmem_limit_bytes=60 * 1024 * 1024
        ),
    )(
        encoder_input, input_gain.reshape(1, D), expand_weight, reduce_weight,
        final_gain.reshape(CHUNKS, 128), decoder_input, query_gain.reshape(1, D), query_weight,
        key_weight, value_weight, mixing_weight, output_gradient,
    )
    return outs[0], outs[1]


def solution(mesh):
    in_specs = (
        P("section", None), P(), P(None, "mp"), P("mp", None), P(), P("section", None), P(),
        P(None, "mp"), P(None, "mp"), P(None, "mp"), P("mp", None), P("section", None),
    )
    out_specs = (P(("section", "mp"), None), P(("section", "mp"), None))
    return jax.shard_map(body, mesh=mesh, in_specs=in_specs, out_specs=out_specs, check_vma=False)
```
